32 devices in a mesh: row: 8 (over z, x), mem: 2 (over core), lev: 2 (over y).
Axes of the slice: x: 2, y: 2, z: 4, core: 2. Of those that a mesh axis runs over, the one named last changes fastest.
Arguments:
- control_fields: bfloat16 [4, 6, 256, 2048], P('mem', 'lev', 'row'), may hold values from -6 to 6
- perturbations: bfloat16 [3, 4, 6, 256, 2048], P(None, 'mem', 'lev', 'row'), may hold values from -3 to 3
- column_taper: bfloat16 [2048, 2048], P('row'), may hold values from -1 to 2, as said below
- row_taper: bfloat16 [256, 256], P('row'), may hold values from -1 to 2, as said below
- courant_numbers: float32 [3, 6, 256, 2048], P(None, 'lev', 'row', 'mem'), may hold values from -0.3 to 0.3
- tracer_slope: float32 [2, 6, 256, 2048], P(None, 'lev', 'row', 'mem'), may hold values from -3 to 3
Outputs:
- increment: float32 [3, 6, 256, 2048], P(None, 'lev', 'row', 'mem')
The draws below stay inside these ranges and needn't reach their ends.
Inputs may be any that keep to these rules, and one draw needn't show every extreme that they name: `column_taper`: A square matrix. `row_taper`: A square matrix.
All inputs are finite; a program needn't handle non-finite values.
Results may differ from the reference program's by a relative error of at most 0.0048.
Values may be sent and summed in bfloat16 or wider, within the bound.
A program may use at most 64 MiB of HBM per device.

```python
import jax
import jax.numpy as jnp
from jax import lax

NX = 2048
STEPS = 4
NY = 256
M = 4
LEV = 6


def banded(key, order):
    first_index = jnp.arange(order)[:, None]
    second_index = jnp.arange(order)[None, :]
    reach = order / 4.0
    noise = jnp.clip(jax.random.normal(key, (order, order), jnp.float32), -4.0, 4.0)
    distance = jnp.abs(first_index - second_index).astype(jnp.float32)
    diagonal = jnp.where(first_index == second_index, 1.0, 0.0).astype(jnp.float32)
    return (diagonal + noise * jnp.exp(-distance / reach) / jnp.sqrt(reach)).astype(jnp.bfloat16)


def draw_column_taper(key, part):
    return banded(jax.random.fold_in(key, 11), NX)


def draw_row_taper(key, part):
    return banded(jax.random.fold_in(key, 23), NY)


def level_of(own_key, shape, pieces, low, top_value):
    gain = 1.0
    for axis_at, parts in pieces:
        heights = jax.random.uniform(jax.random.fold_in(jax.random.fold_in(own_key, 6), axis_at), (parts,), jnp.float32, low / len(pieces), top_value / len(pieces))
        gain = gain * jnp.repeat(jnp.exp(heights), shape[axis_at] // parts).reshape((-1,) + (1,) * (len(shape) - 1 - axis_at))
    return gain


def scatter_about(own_key, dims, width, bound, split=(), held_as=jnp.bfloat16):
    array = jax.random.normal(own_key, dims, jnp.float32) * width
    if len(split) > 0:
        array = level_of(own_key, dims, split, -0.22, 0.18) * array
    return jnp.clip(array, min=-bound, max=bound).astype(held_as)


def setup_inputs(seed: int = 0) -> dict:
    key_list = jax.random.split(jax.random.key(seed), 7)
    return {
        "control_fields": scatter_about(key_list[0], (M, LEV, NY, NX), 1.0, 6.0, ((0, 2), (1, 2), (2, 8))),
        "perturbations": scatter_about(key_list[1], (3, M, LEV, NY, NX), M ** -0.5, 3.0, ((1, 2), (2, 2), (3, 8))),
        "column_taper": draw_column_taper(jax.random.fold_in(key_list[6], 71), 0),
        "row_taper": draw_row_taper(jax.random.fold_in(key_list[6], 71), 0),
        "courant_numbers": jnp.clip(jax.random.uniform(key_list[4], (3, LEV, NY, NX), jnp.float32, -0.3, 0.3) * level_of(key_list[4], (3, LEV, NY, NX), ((1, 2), (2, 8), (3, 2)), -0.4, 0.0), -0.3, 0.3),
        "tracer_slope": scatter_about(key_list[5], (2, LEV, NY, NX), 0.5, 3.0, ((1, 2), (2, 8), (3, 2)), jnp.float32),
    }


def upwind(middle, behind, forward, velocity):
    return jnp.maximum(velocity, 0.0) * (middle - behind) + jnp.minimum(velocity, 0.0) * (forward - middle)


def advance(present, courant_numbers, tracer_slope, padded):
    middle = padded[:, 1:-1, 1:-1, 1:-1]
    change = upwind(middle, padded[:, :-2, 1:-1, 1:-1], padded[:, 2:, 1:-1, 1:-1], courant_numbers[0])
    change = change + upwind(middle, padded[:, 1:-1, :-2, 1:-1], padded[:, 1:-1, 2:, 1:-1], courant_numbers[1])
    change = change + upwind(middle, padded[:, 1:-1, 1:-1, :-2], padded[:, 1:-1, 1:-1, 2:], courant_numbers[2])
    shifted = present - change
    source = present[0] * tracer_slope[0] + present[1] * tracer_slope[1]
    return jnp.concatenate([shifted[:2], shifted[2:] - source[None]], axis=0)


def reference(control_fields, perturbations, column_taper, row_taper, courant_numbers, tracer_slope):
    def per_level(plane):
        first_pass = jnp.dot(plane, column_taper, preferred_element_type=jnp.float32).astype(jnp.bfloat16)
        return jnp.dot(row_taper, first_pass, preferred_element_type=jnp.float32).astype(jnp.bfloat16)

    def accumulate(running, member_pair):
        control_one, perturb_one = member_pair
        localized = lax.map(per_level, control_one)
        return running + perturb_one.astype(jnp.float32) * localized.astype(jnp.float32)[None], None

    starting = jnp.zeros((3,) + control_fields.shape[1:], jnp.float32)
    present, ignored = lax.scan(accumulate, starting, (control_fields, jnp.moveaxis(perturbations, 1, 0)))
    for advect_step in range(STEPS):
        padded = jnp.pad(present, ((0, 0), (1, 1), (1, 1), (1, 1)))
        present = advance(present, courant_numbers, tracer_slope, padded)
    return present
```

```python
import jax
import jax.numpy as jnp
from jax import lax
from jax.sharding import PartitionSpec as P

STEPS = 4


def faces(block, axis, dim):
    count = lax.axis_size(axis)
    forward = [(i, i + 1) for i in range(count - 1)]
    backward = [(target, source) for source, target in forward]
    last = block.shape[dim]
    low = lax.ppermute(lax.slice_in_dim(block, last - 1, last, axis=dim), axis, forward)
    high = lax.ppermute(lax.slice_in_dim(block, 0, 1, axis=dim), axis, backward)
    return low, high


def advance(present, courant_numbers, tracer_slope):
    change = 0.0
    ends = [faces(present, axis, dim) for axis, dim in (("lev", 1), ("row", 2), ("mem", 3))]
    for at, (low, high) in enumerate(ends):
        dim = at + 1
        size = present.shape[dim]
        behind = jnp.concatenate([low, lax.slice_in_dim(present, 0, size - 1, axis=dim)], axis=dim)
        forward = jnp.concatenate([lax.slice_in_dim(present, 1, size, axis=dim), high], axis=dim)
        velocity = courant_numbers[at]
        change = change + (
            jnp.maximum(velocity, 0.0) * (present - behind)
            + jnp.minimum(velocity, 0.0) * (forward - present)
        )
    shifted = present - change
    source = present[0] * tracer_slope[0] + present[1] * tracer_slope[1]
    return jnp.concatenate([shifted[:2], shifted[2:] - source[None]], axis=0)


def on_device(
    control_fields, perturbations, column_taper, row_taper, courant_numbers, tracer_slope
):
    member_count, level_count, row_count, column_count = control_fields.shape
    field_count = member_count * level_count
    mem_count = lax.axis_size("mem")
    mem_at = lax.axis_index("mem")
    width = column_count // mem_count
    own_block = lax.dynamic_slice_in_dim(column_taper, mem_at * width, width, 1)
    taper_columns = lax.all_gather(own_block, "row", axis=0, tiled=True)
    row_whole = lax.all_gather(row_taper, "row", axis=0, tiled=True)
    fields = control_fields.reshape(field_count, row_count, column_count)
    tapered = jnp.einsum(
        "ij,fjc->fic",
        row_whole,
        lax.all_to_all(fields, "row", split_axis=2, concat_axis=1, tiled=True),
        preferred_element_type=jnp.float32,
    )
    tapered = lax.all_to_all(
        tapered.astype(jnp.bfloat16), "row", split_axis=1, concat_axis=2, tiled=True
    )
    weighted = 0.0
    for shift in range(mem_count):
        ring = [(i, (i + shift) % mem_count) for i in range(mem_count)]
        target = lax.rem(mem_at + shift, mem_count)
        part = lax.dynamic_slice_in_dim(perturbations, target * width, width, 4)
        half = tapered
        if shift:
            part = lax.ppermute(part, "mem", ring)
            half = lax.ppermute(half, "mem", ring)
        localized = jnp.dot(
            half.reshape(field_count * row_count, column_count),
            taper_columns,
            preferred_element_type=jnp.float32,
        ).reshape(member_count, level_count, row_count, width)
        for m in range(member_count):
            weighted = weighted + part[:, m].astype(jnp.float32) * localized[m][None]
    present = weighted
    for advect_step in range(STEPS):
        present = advance(present, courant_numbers, tracer_slope)
    return present


def solution(mesh):
    placed = (
        P("mem", "lev", "row", None),
        P(None, "mem", "lev", "row", None),
        P("row", None),
        P("row", None),
        P(None, "lev", "row", "mem"),
        P(None, "lev", "row", "mem"),
    )
    return jax.shard_map(
        on_device,
        mesh=mesh,
        in_specs=placed,
        out_specs=P(None, "lev", "row", "mem"),
        check_vma=False,
    )
```

```python
import jax
import jax.numpy as jnp
from jax import lax
from jax.experimental import pallas as pl
from jax.experimental.pallas import tpu as pltpu
from jax.sharding import PartitionSpec as P

STEPS = 4


MESH = pl.DeviceIdType.MESH
AXES = ("lev", "row", "mem")


def sides():
    found = []
    for at, axis in enumerate(AXES):
        here, count = lax.axis_index(axis), lax.axis_size(axis)
        if count > 1:
            found.append((at, 0, axis, here > 0, here - 1))
            found.append((at, 1, axis, here < count - 1, here + 1))
    return found


def advect_kernel(
    first, courant, slope, out, state, factors, level_send, row_send, level_halo, row_halo,
    column_halo, send_sem, recv_sem,
):
    kinds, levels, rows, width = first.shape
    barrier = pltpu.get_barrier_semaphore()
    neighbours = sides()
    for at, side, axis, there, target in neighbours:

        @pl.when(there)
        def _():
            pl.semaphore_signal(barrier, inc=1, device_id={axis: target}, device_id_type=MESH)

    row_at = lax.broadcasted_iota(jnp.int32, (rows, width), 0)
    column_at = lax.broadcasted_iota(jnp.int32, (rows, width), 1)
    for level in range(levels):
        centre = jnp.ones((rows, width), jnp.float32)
        for at in range(3):
            ahead = jnp.maximum(courant[at, level], 0.0)
            back = jnp.minimum(courant[at, level], 0.0)
            centre = centre - ahead + back
            if at == 1:
                ahead = jnp.where(row_at == 0, 0.0, ahead)
                back = jnp.where(row_at == rows - 1, 0.0, back)
            if at == 2:
                ahead = jnp.where(column_at == 0, 0.0, ahead)
                back = jnp.where(column_at == width - 1, 0.0, back)
            factors[1 + 2 * at, level] = ahead
            factors[2 + 2 * at, level] = back
        factors[0, level] = centre
    for kind in range(kinds):
        for level in range(levels):
            state[0, kind, level] = first[kind, level]
    pl.semaphore_wait(barrier, sum(there.astype(jnp.int32) for _, _, _, there, _ in neighbours))

    def copy_of(step, at, side, axis, target):
        if at == 0:
            source, landing = level_send.at[step, side], level_halo.at[step, 1 - side]
        elif at == 1:
            source, landing = row_send.at[step, side], row_halo.at[step, 1 - side]
        else:
            lanes = pl.ds(0 if side == 0 else width - 128, 128)
            source = state.at[step, :, :, :, lanes]
            landing = column_halo.at[step, 1 - side]
        return pltpu.make_async_remote_copy(
            src_ref=source,
            dst_ref=landing,
            send_sem=send_sem.at[step, 2 * at + side],
            recv_sem=recv_sem.at[step, 2 * at + 1 - side],
            device_id={axis: target},
            device_id_type=MESH,
        )

    def arrival(step, at, side, axis, target):
        landing = (level_halo, row_halo, column_halo)[at].at[step, side]
        return pltpu.make_async_remote_copy(
            src_ref=landing,
            dst_ref=landing,
            send_sem=send_sem.at[step, 2 * at + side],
            recv_sem=recv_sem.at[step, 2 * at + side],
            device_id={axis: target},
            device_id_type=MESH,
        )

    def one_step(step, target_ref):
        for at, side, axis, there, target in neighbours:

            @pl.when(there)
            def _():
                for kind in range(kinds):
                    if at == 0:
                        level_send[step, side, kind] = state[
                            step, kind, 0 if side == 0 else levels - 1
                        ].astype(level_send.dtype)
                    if at == 1:
                        edge = 0 if side == 0 else rows - 1
                        for level in range(levels):
                            row_send[step, side, pl.ds(kind * levels + level, 1)] = state[
                                step, kind, level, pl.ds(edge, 1)
                            ]
                copy_of(step, at, side, axis, target).start()

        for level in range(levels):
            for kind in range(kinds):
                here = state[step, kind, level]
                new = here * factors[0, level]
                new = new + factors[3, level] * pltpu.roll(here, 1, 0)
                new = new - factors[4, level] * pltpu.roll(here, rows - 1, 0)
                new = new + factors[5, level] * pltpu.roll(here, 1, 1)
                new = new - factors[6, level] * pltpu.roll(here, width - 1, 1)
                if level > 0:
                    new = new + factors[1, level] * state[step, kind, level - 1]
                if level < levels - 1:
                    new = new - factors[2, level] * state[step, kind, level + 1]
                if kind == 2:
                    new = new - (
                        state[step, 0, level] * slope[0, level]
                        + state[step, 1, level] * slope[1, level]
                    )
                target_ref[kind, level] = new

        lane_at = lax.broadcasted_iota(jnp.int32, (rows, 128), 1)
        for at, side, axis, there, target in (
            [n for n in neighbours if n[0] == 2]
            + [n for n in neighbours if n[0] == 1]
            + [n for n in neighbours if n[0] == 0]
        ):

            @pl.when(there)
            def _():
                arrival(step, at, side, axis, target).wait_recv()
                for kind in range(kinds):
                    if at == 0:
                        level = 0 if side == 0 else levels - 1
                        term = factors[1 + side, level] * level_halo[step, side, kind].astype(
                            jnp.float32
                        )
                        if side:
                            term = -term
                        target_ref[kind, level] = target_ref[kind, level] + term
                        continue
                    for level in range(levels):
                        if at == 1:
                            edge = pl.ds(0 if side == 0 else rows - 1, 1)
                            speed = courant[1, level, edge]
                            speed = jnp.minimum(speed, 0.0) if side else jnp.maximum(speed, 0.0)
                            term = speed * row_halo[step, side, pl.ds(kind * levels + level, 1)]
                            if side:
                                term = -term
                            target_ref[kind, level, edge] = target_ref[kind, level, edge] + term
                        else:
                            lanes = pl.ds(width - 128 if side else 0, 128)
                            speed = courant[2, level, :, lanes]
                            speed = jnp.minimum(speed, 0.0) if side else jnp.maximum(speed, 0.0)
                            beside = pltpu.roll(
                                column_halo[step, side, kind, level], 127 if side else 1, 1
                            )
                            term = jnp.where(
                                lane_at == (127 if side else 0), speed * beside, 0.0
                            )
                            if side:
                                term = -term
                            target_ref[kind, level, :, lanes] = (
                                target_ref[kind, level, :, lanes] + term
                            )

    @pl.loop(0, STEPS - 1)
    def _(step):
        one_step(step, state.at[step + 1])

    one_step(STEPS - 1, out)

    @pl.loop(0, STEPS)
    def _(step):
        for at, side, axis, there, target in neighbours:

            @pl.when(there)
            def _():
                copy_of(step, at, side, axis, target).wait_send()


def advected(weighted, courant_numbers, tracer_slope):
    kinds, levels, rows, width = weighted.shape
    edges = -(-kinds * levels // 8) * 8
    return pl.pallas_call(
        advect_kernel,
        out_shape=jax.ShapeDtypeStruct(weighted.shape, jnp.float32),
        in_specs=[pl.BlockSpec(memory_space=pltpu.VMEM)] * 3,
        out_specs=pl.BlockSpec(memory_space=pltpu.VMEM),
        scratch_shapes=[
            pltpu.VMEM((STEPS, kinds, levels, rows, width), jnp.float32),
            pltpu.VMEM((7, levels, rows, width), jnp.float32),
            pltpu.VMEM((STEPS, 2, kinds, rows, width), jnp.bfloat16),
            pltpu.VMEM((STEPS, 2, edges, width), jnp.float32),
            pltpu.VMEM((STEPS, 2, kinds, rows, width), jnp.bfloat16),
            pltpu.VMEM((STEPS, 2, edges, width), jnp.float32),
            pltpu.VMEM((STEPS, 2, kinds, levels, rows, 128), jnp.float32),
            pltpu.SemaphoreType.DMA((STEPS, 6)),
            pltpu.SemaphoreType.DMA((STEPS, 6)),
        ],
        compiler_params=pltpu.CompilerParams(
            collective_id=1, has_side_effects=True, vmem_limit_bytes=48 << 20
        ),
        name="advect",
    )(weighted, courant_numbers, tracer_slope)


def on_device(
    control_fields, perturbations, column_taper, row_taper, courant_numbers, tracer_slope
):
    member_count, level_count, row_count, column_count = control_fields.shape
    field_count = member_count * level_count
    mem_count = lax.axis_size("mem")
    mem_at = lax.axis_index("mem")
    width = column_count // mem_count
    own_block = lax.dynamic_slice_in_dim(column_taper, mem_at * width, width, 1)
    taper_columns = lax.all_gather(own_block, "row", axis=0, tiled=True)
    row_whole = lax.all_gather(row_taper, "row", axis=0, tiled=True)
    fields = control_fields.reshape(field_count, row_count, column_count)
    tapered = jnp.einsum(
        "ij,fjc->fic",
        row_whole,
        lax.all_to_all(fields, "row", split_axis=2, concat_axis=1, tiled=True),
        preferred_element_type=jnp.float32,
    )
    tapered = lax.all_to_all(
        tapered.astype(jnp.bfloat16), "row", split_axis=1, concat_axis=2, tiled=True
    )
    weighted = 0.0
    for shift in range(mem_count):
        ring = [(i, (i + shift) % mem_count) for i in range(mem_count)]
        target = lax.rem(mem_at + shift, mem_count)
        part = lax.dynamic_slice_in_dim(perturbations, target * width, width, 4)
        half = tapered
        if shift:
            part = lax.ppermute(part, "mem", ring)
            half = lax.ppermute(half, "mem", ring)
        localized = jnp.dot(
            half.reshape(field_count * row_count, column_count),
            taper_columns,
            preferred_element_type=jnp.float32,
        ).reshape(member_count, level_count, row_count, width)
        for m in range(member_count):
            weighted = weighted + part[:, m].astype(jnp.float32) * localized[m][None]
    return advected(weighted, courant_numbers, tracer_slope)


def solution(mesh):
    placed = (
        P("mem", "lev", "row", None),
        P(None, "mem", "lev", "row", None),
        P("row", None),
        P("row", None),
        P(None, "lev", "row", "mem"),
        P(None, "lev", "row", "mem"),
    )
    return jax.shard_map(
        on_device,
        mesh=mesh,
        in_specs=placed,
        out_specs=P(None, "lev", "row", "mem"),
        check_vma=False,
    )
```

```python
import jax
import jax.numpy as jnp
from jax import lax
from jax.experimental import pallas as pl
from jax.experimental.pallas import tpu as pltpu
from jax.sharding import PartitionSpec as P

STEPS = 4


MESH = pl.DeviceIdType.MESH
AXES = ("lev", "row", "mem")


def sides():
    found = []
    for at, axis in enumerate(AXES):
        here, count = lax.axis_index(axis), lax.axis_size(axis)
        if count > 1:
            found.append((at, 0, axis, here > 0, here - 1))
            found.append((at, 1, axis, here < count - 1, here + 1))
    return found


def advect_kernel(
    first, courant, slope, out, state, factors, level_send, row_send, level_halo, row_halo,
    column_halo, send_sem, recv_sem,
):
    kinds, levels, rows, width = first.shape
    barrier = pltpu.get_barrier_semaphore()
    neighbours = sides()
    for at, side, axis, there, target in neighbours:

        @pl.when(there)
        def _():
            pl.semaphore_signal(barrier, inc=1, device_id={axis: target}, device_id_type=MESH)

    row_at = lax.broadcasted_iota(jnp.int32, (rows, width), 0)
    column_at = lax.broadcasted_iota(jnp.int32, (rows, width), 1)
    for level in range(levels):
        centre = jnp.ones((rows, width), jnp.float32)
        for at in range(3):
            ahead = jnp.maximum(courant[at, level], 0.0)
            back = jnp.minimum(courant[at, level], 0.0)
            centre = centre - ahead + back
            if at == 1:
                ahead = jnp.where(row_at == 0, 0.0, ahead)
                back = jnp.where(row_at == rows - 1, 0.0, back)
            if at == 2:
                ahead = jnp.where(column_at == 0, 0.0, ahead)
                back = jnp.where(column_at == width - 1, 0.0, back)
            factors[1 + 2 * at, level] = ahead
            factors[2 + 2 * at, level] = back
        factors[0, level] = centre
    for kind in range(kinds):
        for level in range(levels):
            state[0, kind, level] = first[kind, level]
    pl.semaphore_wait(barrier, sum(there.astype(jnp.int32) for _, _, _, there, _ in neighbours))

    def copy_of(step, at, side, axis, target):
        if at == 0:
            source, landing = level_send.at[step, side], level_halo.at[step, 1 - side]
        elif at == 1:
            source, landing = row_send.at[step, side], row_halo.at[step, 1 - side]
        else:
            lanes = pl.ds(0 if side == 0 else width - 128, 128)
            source = state.at[step, :, :, :, lanes]
            landing = column_halo.at[step, 1 - side]
        return pltpu.make_async_remote_copy(
            src_ref=source,
            dst_ref=landing,
            send_sem=send_sem.at[step, 2 * at + side],
            recv_sem=recv_sem.at[step, 2 * at + 1 - side],
            device_id={axis: target},
            device_id_type=MESH,
        )

    def arrival(step, at, side, axis, target):
        landing = (level_halo, row_halo, column_halo)[at].at[step, side]
        return pltpu.make_async_remote_copy(
            src_ref=landing,
            dst_ref=landing,
            send_sem=send_sem.at[step, 2 * at + side],
            recv_sem=recv_sem.at[step, 2 * at + side],
            device_id={axis: target},
            device_id_type=MESH,
        )

    def one_step(step, target_ref):
        for at, side, axis, there, target in neighbours:

            @pl.when(there)
            def _():
                for kind in range(kinds):
                    if at == 0:
                        level_send[step, side, kind] = state[
                            step, kind, 0 if side == 0 else levels - 1
                        ].astype(level_send.dtype)
                    if at == 1:
                        edge = 0 if side == 0 else rows - 1
                        for level in range(levels):
                            row_send[step, side, pl.ds(kind * levels + level, 1)] = state[
                                step, kind, level, pl.ds(edge, 1)
                            ]
                copy_of(step, at, side, axis, target).start()

        for level in range(levels):
            for kind in range(kinds):
                here = state[step, kind, level]
                new = here * factors[0, level]
                new = new + factors[3, level] * pltpu.roll(here, 1, 0)
                new = new - factors[4, level] * pltpu.roll(here, rows - 1, 0)
                new = new + factors[5, level] * pltpu.roll(here, 1, 1)
                new = new - factors[6, level] * pltpu.roll(here, width - 1, 1)
                if level > 0:
                    new = new + factors[1, level] * state[step, kind, level - 1]
                if level < levels - 1:
                    new = new - factors[2, level] * state[step, kind, level + 1]
                if kind == 2:
                    new = new - (
                        state[step, 0, level] * slope[0, level]
                        + state[step, 1, level] * slope[1, level]
                    )
                target_ref[kind, level] = new

        lane_at = lax.broadcasted_iota(jnp.int32, (rows, 128), 1)
        for at, side, axis, there, target in (
            [n for n in neighbours if n[0] == 2]
            + [n for n in neighbours if n[0] == 1]
            + [n for n in neighbours if n[0] == 0]
        ):

            @pl.when(there)
            def _():
                arrival(step, at, side, axis, target).wait_recv()
                for kind in range(kinds):
                    if at == 0:
                        level = 0 if side == 0 else levels - 1
                        term = factors[1 + side, level] * level_halo[step, side, kind].astype(
                            jnp.float32
                        )
                        if side:
                            term = -term
                        target_ref[kind, level] = target_ref[kind, level] + term
                        continue
                    for level in range(levels):
                        if at == 1:
                            edge = pl.ds(0 if side == 0 else rows - 1, 1)
                            speed = courant[1, level, edge]
                            speed = jnp.minimum(speed, 0.0) if side else jnp.maximum(speed, 0.0)
                            term = speed * row_halo[step, side, pl.ds(kind * levels + level, 1)]
                            if side:
                                term = -term
                            target_ref[kind, level, edge] = target_ref[kind, level, edge] + term
                        else:
                            lanes = pl.ds(width - 128 if side else 0, 128)
                            speed = courant[2, level, :, lanes]
                            speed = jnp.minimum(speed, 0.0) if side else jnp.maximum(speed, 0.0)
                            beside = pltpu.roll(
                                column_halo[step, side, kind, level], 127 if side else 1, 1
                            )
                            term = jnp.where(
                                lane_at == (127 if side else 0), speed * beside, 0.0
                            )
                            if side:
                                term = -term
                            target_ref[kind, level, :, lanes] = (
                                target_ref[kind, level, :, lanes] + term
                            )

    @pl.loop(0, STEPS - 1)
    def _(step):
        one_step(step, state.at[step + 1])

    one_step(STEPS - 1, out)

    @pl.loop(0, STEPS)
    def _(step):
        for at, side, axis, there, target in neighbours:

            @pl.when(there)
            def _():
                copy_of(step, at, side, axis, target).wait_send()


def advected(weighted, courant_numbers, tracer_slope):
    kinds, levels, rows, width = weighted.shape
    edges = -(-kinds * levels // 8) * 8
    return pl.pallas_call(
        advect_kernel,
        out_shape=jax.ShapeDtypeStruct(weighted.shape, jnp.float32),
        in_specs=[pl.BlockSpec(memory_space=pltpu.VMEM)] * 3,
        out_specs=pl.BlockSpec(memory_space=pltpu.VMEM),
        scratch_shapes=[
            pltpu.VMEM((STEPS, kinds, levels, rows, width), jnp.float32),
            pltpu.VMEM((7, levels, rows, width), jnp.float32),
            pltpu.VMEM((STEPS, 2, kinds, rows, width), jnp.bfloat16),
            pltpu.VMEM((STEPS, 2, edges, width), jnp.float32),
            pltpu.VMEM((STEPS, 2, kinds, rows, width), jnp.bfloat16),
            pltpu.VMEM((STEPS, 2, edges, width), jnp.float32),
            pltpu.VMEM((STEPS, 2, kinds, levels, rows, 128), jnp.float32),
            pltpu.SemaphoreType.DMA((STEPS, 6)),
            pltpu.SemaphoreType.DMA((STEPS, 6)),
        ],
        compiler_params=pltpu.CompilerParams(
            collective_id=1, has_side_effects=True, vmem_limit_bytes=48 << 20
        ),
        name="advect",
    )(weighted, courant_numbers, tracer_slope)


def localize_kernel(
    control, pert, taper, row_part, out, gathered, row_all, staged, halves, taper_all, pert_all,
    total, one_send, one_recv, row_send, row_recv, two_send, two_recv, pass_send, pass_recv,
    pert_send, pert_recv, ring_send, ring_recv, lev_send, lev_recv, own_sem,
):
    count, mems, levs = (lax.axis_size(axis) for axis in ("row", "mem", "lev"))
    me, mem_at, lev_at = (lax.axis_index(axis) for axis in ("row", "mem", "lev"))
    fields, rows, depth = control.shape[1:]
    kinds, members, levels = pert.shape[:3]
    width = out.shape[3]
    chains = ring_send.shape[0]
    lanes, share = width // chains, depth // levs
    half = count // 2

    def order(place):
        place = (place + 2 * count) % count
        late = place // half
        return (1 - late) * 2 * place + late * (2 * (count - 1 - place) + 1)

    place = (1 - me % 2) * (me // 2) + (me % 2) * (count - 1 - me // 2)

    def remote(source, landing, sent, landed, **target):
        return pltpu.make_async_remote_copy(
            src_ref=source, dst_ref=landing, send_sem=sent, recv_sem=landed,
            device_id=target, device_id_type=MESH,
        )

    def own_columns(at):
        return pl.ds(pl.multiple_of(at * width, width), width)

    def one(peer, slot):
        return remote(control.at[peer], gathered.at[slot], one_send.at[peer], one_recv.at[slot], row=peer)

    def row(peer, slot):
        return remote(row_part, row_all.at[slot], row_send.at[peer], row_recv.at[slot], row=peer)

    def two(peer, slot):
        return remote(
            staged.at[peer], halves.at[mem_at, slot], two_send.at[peer], two_recv.at[slot], row=peer
        )

    def onward(peer, slot, place_of):
        return remote(
            halves.at[place_of, slot], halves.at[place_of, slot], pass_send.at[peer, slot],
            pass_recv.at[place_of, slot], mem=peer,
        )

    def pert_copy(peer, slot):
        return remote(
            pert.at[:, :, :, :, own_columns(peer)], pert_all.at[slot], pert_send.at[peer],
            pert_recv.at[slot], mem=peer,
        )

    def piece(chain, origin, lev):
        return taper_all.at[
            origin, pl.ds(pl.multiple_of(lev * share, share), share), pl.ds(chain * lanes, lanes)
        ]

    def ring(chain, hop, sending):
        way = 1 - 2 * (chain % 2)
        origin = order(place - way * hop) if sending else order(place - way * (hop + 1))
        part = piece(chain, origin, lev_at)
        return remote(part, part, ring_send.at[chain, hop], ring_recv.at[chain, hop], row=order(place + way))

    def across(chain, hop, shift, sending):
        way = 1 - 2 * (chain % 2)
        origin = order(place - way * (hop + 1))
        peer = (lev_at + shift) % levs
        source = (lev_at + levs - shift) % levs
        part = piece(chain, origin, lev_at if sending else source)
        return remote(
            part, part, lev_send.at[chain, hop, shift - 1], lev_recv.at[chain, hop, shift - 1], lev=peer
        )

    def ring_step(hop, last):
        for chain in range(chains):
            ring(chain, hop - 1, False).wait_recv()
            if not last:
                ring(chain, hop, True).start()
            for shift in range(1, levs):
                across(chain, hop - 1, shift, True).start()

    barrier = pltpu.get_barrier_semaphore()
    for axis, here, size in (("row", me, count), ("mem", mem_at, mems), ("lev", lev_at, levs)):

        @pl.loop(1, size)
        def _(shift):
            pl.semaphore_signal(
                barrier, inc=1, device_id={axis: (here + shift) % size}, device_id_type=MESH
            )

    own_taper = pltpu.make_async_copy(taper.at[:, own_columns(mem_at)], taper_all.at[me], own_sem.at[0])
    own_taper.start()
    own_pert = pltpu.make_async_copy(
        pert.at[:, :, :, :, own_columns(mem_at)], pert_all.at[mem_at], own_sem.at[1]
    )
    own_pert.start()
    gathered[me] = control[me]
    row_all[me] = row_part[...]
    own_taper.wait()
    pl.semaphore_wait(barrier, count + mems + levs - 3)

    @pl.loop(1, count)
    def _(shift):
        peer = (me + shift) % count
        row(peer, me).start()
        one(peer, me).start()

    for chain in range(chains):
        ring(chain, 0, True).start()

    @pl.loop(1, mems)
    def _(shift):
        pert_copy((mem_at + shift) % mems, mem_at).start()

    ring_step(1, count == 2)

    @pl.loop(1, count)
    def _(shift):
        peer = (me + shift) % count
        row(peer, peer).wait_recv()
        one(peer, peer).wait_recv()

    row_whole = row_all[...].reshape(count * rows, count * rows)

    @pl.loop(0, fields)
    def _(field):
        tapered = jnp.dot(
            row_whole,
            gathered[:, field].reshape(count * rows, depth),
            preferred_element_type=jnp.float32,
        )
        staged[:, field] = tapered.astype(jnp.bfloat16).reshape(count, rows, depth)

    @pl.loop(1, count)
    def _(shift):
        two((me + shift) % count, me).start()

    halves[mem_at, me] = staged[me]

    @pl.loop(1, mems)
    def _(shift):
        onward((mem_at + shift) % mems, me, mem_at).start()

    if count > 2:

        @pl.loop(2, count - 1)
        def _(hop):
            ring_step(hop, False)

        ring_step(count - 1, True)

    @pl.loop(1, count)
    def _(shift):
        slot = (me + shift) % count
        two(slot, slot).wait_recv()

        @pl.loop(1, mems)
        def _(step):
            onward((mem_at + step) % mems, slot, mem_at).start()

    @pl.loop(1, mems)
    def _(step):
        peer = (mem_at + step) % mems
        pert_copy(peer, peer).wait_recv()

        @pl.loop(0, count)
        def _(slot):
            onward(peer, slot, peer).wait_recv()

    @pl.loop(0, count - 1)
    def _(hop):
        for chain in range(chains):
            for shift in range(1, levs):
                across(chain, hop, shift, False).wait_recv()

    total[...] = jnp.zeros_like(total)

    @pl.loop(0, count)
    def _(slot):
        total[...] += jnp.dot(
            halves[:, slot].reshape(mems * fields * rows, depth),
            taper_all[slot],
            preferred_element_type=jnp.float32,
        )

    own_pert.wait()
    for level in range(levels):
        for kind in range(kinds):
            weighted = jnp.zeros((rows, width), jnp.float32)
            for mem in range(mems):
                for member in range(members):
                    at = ((mem * members + member) * levels + level) * rows
                    weighted = weighted + pert_all[mem, kind, member, level].astype(
                        jnp.float32
                    ) * total[pl.ds(at, rows)]
            out[kind, level] = weighted

    @pl.loop(1, count)
    def _(shift):
        peer = (me + shift) % count
        row(peer, me).wait_send()
        one(peer, me).wait_send()
        two(peer, me).wait_send()

    @pl.loop(1, mems)
    def _(shift):
        peer = (mem_at + shift) % mems
        pert_copy(peer, mem_at).wait_send()

        @pl.loop(0, count)
        def _(slot):
            onward(peer, slot, mem_at).wait_send()

    @pl.loop(0, count - 1)
    def _(hop):
        for chain in range(chains):
            ring(chain, hop, True).wait_send()
            for shift in range(1, levs):
                across(chain, hop, shift, True).wait_send()


def localized(control_fields, perturbations, column_taper, row_taper):
    members, levels, rows, columns = control_fields.shape
    kinds = perturbations.shape[0]
    count, mems, levs = (lax.axis_size(axis) for axis in ("row", "mem", "lev"))
    fields, depth, width = members * levels, columns // count, columns // mems
    split = control_fields.reshape(fields, rows, count, depth).transpose(2, 0, 1, 3)
    chains = 4 if width % 512 == 0 else 2
    low, dma = jnp.bfloat16, pltpu.SemaphoreType.DMA
    return pl.pallas_call(
        localize_kernel,
        out_shape=jax.ShapeDtypeStruct((kinds, levels, rows, width), jnp.float32),
        in_specs=[pl.BlockSpec(memory_space=pltpu.VMEM)] * 4,
        out_specs=pl.BlockSpec(memory_space=pltpu.VMEM),
        scratch_shapes=[
            pltpu.VMEM((count, fields, rows, depth), low),
            pltpu.VMEM((count, rows, count * rows), low),
            pltpu.VMEM((count, fields, rows, depth), low),
            pltpu.VMEM((mems, count, fields, rows, depth), low),
            pltpu.VMEM((count, depth, width), low),
            pltpu.VMEM((mems, kinds, members, levels, rows, width), low),
            pltpu.VMEM((mems * fields * rows, width), jnp.float32),
            dma((count,)), dma((count,)), dma((count,)), dma((count,)), dma((count,)), dma((count,)),
            dma((mems, count)), dma((mems, count)), dma((mems,)), dma((mems,)),
            dma((chains, count)), dma((chains, count)),
            dma((chains, count, levs)), dma((chains, count, levs)), dma((2,)),
        ],
        compiler_params=pltpu.CompilerParams(
            collective_id=0, has_side_effects=True, vmem_limit_bytes=56 << 20
        ),
        name="localize",
    )(split, perturbations, column_taper, row_taper)


def on_device(
    control_fields, perturbations, column_taper, row_taper, courant_numbers, tracer_slope
):
    weighted = localized(control_fields, perturbations, column_taper, row_taper)
    return advected(weighted, courant_numbers, tracer_slope)


def solution(mesh):
    placed = (
        P("mem", "lev", "row", None),
        P(None, "mem", "lev", "row", None),
        P("row", None),
        P("row", None),
        P(None, "lev", "row", "mem"),
        P(None, "lev", "row", "mem"),
    )
    return jax.shard_map(
        on_device,
        mesh=mesh,
        in_specs=placed,
        out_specs=P(None, "lev", "row", "mem"),
        check_vma=False,
    )
```

```python
import jax
import jax.numpy as jnp
from jax import lax
from jax.experimental import pallas as pl
from jax.experimental.pallas import tpu as pltpu
from jax.sharding import PartitionSpec as P

STEPS = 4


MESH = pl.DeviceIdType.MESH
AXES = ("lev", "row", "mem")


def sides():
    found = []
    for at, axis in enumerate(AXES):
        here, count = lax.axis_index(axis), lax.axis_size(axis)
        if count > 1:
            found.append((at, 0, axis, here > 0, here - 1))
            found.append((at, 1, axis, here < count - 1, here + 1))
    return found


def advect_kernel(
    first, courant, slope, out, state, factors, level_send, row_send, level_halo, row_halo,
    column_halo, send_sem, recv_sem,
):
    kinds, levels, rows, width = first.shape
    barrier = pltpu.get_barrier_semaphore()
    neighbours = sides()
    for at, side, axis, there, target in neighbours:

        @pl.when(there)
        def _():
            pl.semaphore_signal(barrier, inc=1, device_id={axis: target}, device_id_type=MESH)

    row_at = lax.broadcasted_iota(jnp.int32, (rows, width), 0)
    column_at = lax.broadcasted_iota(jnp.int32, (rows, width), 1)
    for level in range(levels):
        centre = jnp.ones((rows, width), jnp.float32)
        for at in range(3):
            ahead = jnp.maximum(courant[at, level], 0.0)
            back = jnp.minimum(courant[at, level], 0.0)
            centre = centre - ahead + back
            if at == 1:
                ahead = jnp.where(row_at == 0, 0.0, ahead)
                back = jnp.where(row_at == rows - 1, 0.0, back)
            if at == 2:
                ahead = jnp.where(column_at == 0, 0.0, ahead)
                back = jnp.where(column_at == width - 1, 0.0, back)
            factors[1 + 2 * at, level] = ahead
            factors[2 + 2 * at, level] = back
        factors[0, level] = centre
    for kind in range(kinds):
        for level in range(levels):
            state[0, kind, level] = first[kind, level]
    pl.semaphore_wait(barrier, sum(there.astype(jnp.int32) for _, _, _, there, _ in neighbours))

    def copy_of(step, at, side, axis, target):
        if at == 0:
            source, landing = level_send.at[step, side], level_halo.at[step, 1 - side]
        elif at == 1:
            source, landing = row_send.at[step, side], row_halo.at[step, 1 - side]
        else:
            lanes = pl.ds(0 if side == 0 else width - 128, 128)
            source = state.at[step, :, :, :, lanes]
            landing = column_halo.at[step, 1 - side]
        return pltpu.make_async_remote_copy(
            src_ref=source,
            dst_ref=landing,
            send_sem=send_sem.at[step, 2 * at + side],
            recv_sem=recv_sem.at[step, 2 * at + 1 - side],
            device_id={axis: target},
            device_id_type=MESH,
        )

    def arrival(step, at, side, axis, target):
        landing = (level_halo, row_halo, column_halo)[at].at[step, side]
        return pltpu.make_async_remote_copy(
            src_ref=landing,
            dst_ref=landing,
            send_sem=send_sem.at[step, 2 * at + side],
            recv_sem=recv_sem.at[step, 2 * at + side],
            device_id={axis: target},
            device_id_type=MESH,
        )

    def one_step(step, target_ref):
        for at, side, axis, there, target in neighbours:

            @pl.when(there)
            def _():
                for kind in range(kinds):
                    if at == 0:
                        level_send[step, side, kind] = state[
                            step, kind, 0 if side == 0 else levels - 1
                        ].astype(level_send.dtype)
                    if at == 1:
                        edge = 0 if side == 0 else rows - 1
                        for level in range(levels):
                            row_send[step, side, pl.ds(kind * levels + level, 1)] = state[
                                step, kind, level, pl.ds(edge, 1)
                            ]
                copy_of(step, at, side, axis, target).start()

        for level in range(levels):
            for kind in range(kinds):
                here = state[step, kind, level]
                new = here * factors[0, level]
                new = new + factors[3, level] * pltpu.roll(here, 1, 0)
                new = new - factors[4, level] * pltpu.roll(here, rows - 1, 0)
                new = new + factors[5, level] * pltpu.roll(here, 1, 1)
                new = new - factors[6, level] * pltpu.roll(here, width - 1, 1)
                if level > 0:
                    new = new + factors[1, level] * state[step, kind, level - 1]
                if level < levels - 1:
                    new = new - factors[2, level] * state[step, kind, level + 1]
                if kind == 2:
                    new = new - (
                        state[step, 0, level] * slope[0, level]
                        + state[step, 1, level] * slope[1, level]
                    )
                target_ref[kind, level] = new

        lane_at = lax.broadcasted_iota(jnp.int32, (rows, 128), 1)
        for at, side, axis, there, target in (
            [n for n in neighbours if n[0] == 2]
            + [n for n in neighbours if n[0] == 1]
            + [n for n in neighbours if n[0] == 0]
        ):

            @pl.when(there)
            def _():
                arrival(step, at, side, axis, target).wait_recv()
                for kind in range(kinds):
                    if at == 0:
                        level = 0 if side == 0 else levels - 1
                        term = factors[1 + side, level] * level_halo[step, side, kind].astype(
                            jnp.float32
                        )
                        if side:
                            term = -term
                        target_ref[kind, level] = target_ref[kind, level] + term
                        continue
                    for level in range(levels):
                        if at == 1:
                            edge = pl.ds(0 if side == 0 else rows - 1, 1)
                            speed = courant[1, level, edge]
                            speed = jnp.minimum(speed, 0.0) if side else jnp.maximum(speed, 0.0)
                            term = speed * row_halo[step, side, pl.ds(kind * levels + level, 1)]
                            if side:
                                term = -term
                            target_ref[kind, level, edge] = target_ref[kind, level, edge] + term
                        else:
                            lanes = pl.ds(width - 128 if side else 0, 128)
                            speed = courant[2, level, :, lanes]
                            speed = jnp.minimum(speed, 0.0) if side else jnp.maximum(speed, 0.0)
                            beside = pltpu.roll(
                                column_halo[step, side, kind, level], 127 if side else 1, 1
                            )
                            term = jnp.where(
                                lane_at == (127 if side else 0), speed * beside, 0.0
                            )
                            if side:
                                term = -term
                            target_ref[kind, level, :, lanes] = (
                                target_ref[kind, level, :, lanes] + term
                            )

    @pl.loop(0, STEPS - 1)
    def _(step):
        one_step(step, state.at[step + 1])

    one_step(STEPS - 1, out)

    @pl.loop(0, STEPS)
    def _(step):
        for at, side, axis, there, target in neighbours:

            @pl.when(there)
            def _():
                copy_of(step, at, side, axis, target).wait_send()


def advected(weighted, courant_numbers, tracer_slope):
    kinds, levels, rows, width = weighted.shape
    edges = -(-kinds * levels // 8) * 8
    return pl.pallas_call(
        advect_kernel,
        out_shape=jax.ShapeDtypeStruct(weighted.shape, jnp.float32),
        in_specs=[pl.BlockSpec(memory_space=pltpu.VMEM)] * 3,
        out_specs=pl.BlockSpec(memory_space=pltpu.VMEM),
        scratch_shapes=[
            pltpu.VMEM((STEPS, kinds, levels, rows, width), jnp.float32),
            pltpu.VMEM((7, levels, rows, width), jnp.float32),
            pltpu.VMEM((STEPS, 2, kinds, rows, width), jnp.bfloat16),
            pltpu.VMEM((STEPS, 2, edges, width), jnp.float32),
            pltpu.VMEM((STEPS, 2, kinds, rows, width), jnp.bfloat16),
            pltpu.VMEM((STEPS, 2, edges, width), jnp.float32),
            pltpu.VMEM((STEPS, 2, kinds, levels, rows, 128), jnp.float32),
            pltpu.SemaphoreType.DMA((STEPS, 6)),
            pltpu.SemaphoreType.DMA((STEPS, 6)),
        ],
        compiler_params=pltpu.CompilerParams(
            collective_id=1, has_side_effects=True, vmem_limit_bytes=48 << 20
        ),
        name="advect",
    )(weighted, courant_numbers, tracer_slope)


def localize_kernel(
    control, pert, taper, row_part, out, gathered, row_all, staged, halves, taper_all, pert_all,
    total, one_send, one_recv, row_send, row_recv, two_send, two_recv, pass_send, pass_recv,
    pert_send, pert_recv, ring_send, ring_recv, lev_send, lev_recv, own_sem,
):
    count, mems, levs = (lax.axis_size(axis) for axis in ("row", "mem", "lev"))
    me, mem_at, lev_at = (lax.axis_index(axis) for axis in ("row", "mem", "lev"))
    fields, rows, depth = control.shape[1:]
    kinds, members, levels = pert.shape[:3]
    width = out.shape[3]
    chains = ring_send.shape[0]
    lanes, share = width // chains, depth // levs
    half = count // 2

    def order(place):
        place = (place + 2 * count) % count
        late = place // half
        return (1 - late) * 2 * place + late * (2 * (count - 1 - place) + 1)

    place = (1 - me % 2) * (me // 2) + (me % 2) * (count - 1 - me // 2)

    def remote(source, landing, sent, landed, **target):
        return pltpu.make_async_remote_copy(
            src_ref=source, dst_ref=landing, send_sem=sent, recv_sem=landed,
            device_id=target, device_id_type=MESH,
        )

    def own_columns(at):
        return pl.ds(pl.multiple_of(at * width, width), width)

    def one(peer, slot):
        return remote(control.at[peer], gathered.at[slot], one_send.at[peer], one_recv.at[slot], row=peer)

    def row(peer, slot):
        return remote(row_part, row_all.at[slot], row_send.at[peer], row_recv.at[slot], row=peer)

    def two(peer, slot):
        return remote(
            staged.at[peer], halves.at[mem_at, slot], two_send.at[peer], two_recv.at[slot], row=peer
        )

    def onward(peer, slot, place_of):
        return remote(
            halves.at[place_of, slot], halves.at[place_of, slot], pass_send.at[peer, slot],
            pass_recv.at[place_of, slot], mem=peer,
        )

    def pert_copy(peer, slot):
        return remote(
            pert.at[:, :, :, :, own_columns(peer)], pert_all.at[slot], pert_send.at[peer],
            pert_recv.at[slot], mem=peer,
        )

    def piece(chain, origin, lev):
        return taper_all.at[
            origin, pl.ds(pl.multiple_of(lev * share, share), share), pl.ds(chain * lanes, lanes)
        ]

    def ring(chain, hop, sending):
        way = 1 - 2 * (chain % 2)
        origin = order(place - way * hop) if sending else order(place - way * (hop + 1))
        part = piece(chain, origin, lev_at)
        return remote(part, part, ring_send.at[chain, hop], ring_recv.at[chain, hop], row=order(place + way))

    def across(chain, hop, shift, sending):
        way = 1 - 2 * (chain % 2)
        origin = order(place - way * (hop + 1))
        peer = (lev_at + shift) % levs
        source = (lev_at + levs - shift) % levs
        part = piece(chain, origin, lev_at if sending else source)
        return remote(
            part, part, lev_send.at[chain, hop, shift - 1], lev_recv.at[chain, hop, shift - 1], lev=peer
        )

    def ring_step(hop, last):
        for chain in range(chains):
            ring(chain, hop - 1, False).wait_recv()
            if not last:
                ring(chain, hop, True).start()
            for shift in range(1, levs):
                across(chain, hop - 1, shift, True).start()

    barrier = pltpu.get_barrier_semaphore()
    for axis, here, size in (("row", me, count), ("mem", mem_at, mems), ("lev", lev_at, levs)):

        @pl.loop(1, size)
        def _(shift):
            pl.semaphore_signal(
                barrier, inc=1, device_id={axis: (here + shift) % size}, device_id_type=MESH
            )

    own_taper = pltpu.make_async_copy(taper.at[:, own_columns(mem_at)], taper_all.at[me], own_sem.at[0])
    own_taper.start()
    own_pert = pltpu.make_async_copy(
        pert.at[:, :, :, :, own_columns(mem_at)], pert_all.at[mem_at], own_sem.at[1]
    )
    own_pert.start()
    gathered[me] = control[me]
    row_all[me] = row_part[...]
    own_taper.wait()
    pl.semaphore_wait(barrier, count + mems + levs - 3)

    for chain in range(chains):
        ring(chain, 0, True).start()

    @pl.loop(1, count)
    def _(shift):
        peer = (me + shift) % count
        row(peer, me).start()
        one(peer, me).start()

    @pl.loop(1, mems)
    def _(shift):
        pert_copy((mem_at + shift) % mems, mem_at).start()

    early = max(1, min(3, count - 2))
    for hop in range(1, early + 1):
        ring_step(hop, count == 2)

    @pl.loop(1, count)
    def _(shift):
        peer = (me + shift) % count
        row(peer, peer).wait_recv()
        one(peer, peer).wait_recv()

    row_whole = row_all[...].reshape(count * rows, count * rows)

    @pl.loop(0, fields)
    def _(field):
        tapered = jnp.dot(
            row_whole,
            gathered[:, field].reshape(count * rows, depth),
            preferred_element_type=jnp.float32,
        )
        staged[:, field] = tapered.astype(jnp.bfloat16).reshape(count, rows, depth)

    @pl.loop(1, count)
    def _(shift):
        two((me + shift) % count, me).start()

    halves[mem_at, me] = staged[me]

    @pl.loop(1, mems)
    def _(shift):
        onward((mem_at + shift) % mems, me, mem_at).start()

    if count > 2:

        @pl.loop(early + 1, count - 1)
        def _(hop):
            ring_step(hop, False)

        ring_step(count - 1, True)

    @pl.loop(1, count)
    def _(shift):
        slot = (me + shift) % count
        two(slot, slot).wait_recv()

        @pl.loop(1, mems)
        def _(step):
            onward((mem_at + step) % mems, slot, mem_at).start()

    @pl.loop(1, mems)
    def _(step):
        peer = (mem_at + step) % mems
        pert_copy(peer, peer).wait_recv()

        @pl.loop(0, count)
        def _(slot):
            onward(peer, slot, peer).wait_recv()

    @pl.loop(0, count - 1)
    def _(hop):
        for chain in range(chains):
            for shift in range(1, levs):
                across(chain, hop, shift, False).wait_recv()

    total[...] = jnp.zeros_like(total)

    @pl.loop(0, count)
    def _(slot):
        total[...] += jnp.dot(
            halves[:, slot].reshape(mems * fields * rows, depth),
            taper_all[slot],
            preferred_element_type=jnp.float32,
        )

    own_pert.wait()
    for level in range(levels):
        for kind in range(kinds):
            weighted = jnp.zeros((rows, width), jnp.float32)
            for mem in range(mems):
                for member in range(members):
                    at = ((mem * members + member) * levels + level) * rows
                    weighted = weighted + pert_all[mem, kind, member, level].astype(
                        jnp.float32
                    ) * total[pl.ds(at, rows)]
            out[kind, level] = weighted

    @pl.loop(1, count)
    def _(shift):
        peer = (me + shift) % count
        row(peer, me).wait_send()
        one(peer, me).wait_send()
        two(peer, me).wait_send()

    @pl.loop(1, mems)
    def _(shift):
        peer = (mem_at + shift) % mems
        pert_copy(peer, mem_at).wait_send()

        @pl.loop(0, count)
        def _(slot):
            onward(peer, slot, mem_at).wait_send()

    @pl.loop(0, count - 1)
    def _(hop):
        for chain in range(chains):
            ring(chain, hop, True).wait_send()
            for shift in range(1, levs):
                across(chain, hop, shift, True).wait_send()


def localized(control_fields, perturbations, column_taper, row_taper):
    members, levels, rows, columns = control_fields.shape
    kinds = perturbations.shape[0]
    count, mems, levs = (lax.axis_size(axis) for axis in ("row", "mem", "lev"))
    fields, depth, width = members * levels, columns // count, columns // mems
    split = control_fields.reshape(fields, rows, count, depth).transpose(2, 0, 1, 3)
    chains = 4 if width % 512 == 0 else 2
    low, dma = jnp.bfloat16, pltpu.SemaphoreType.DMA
    return pl.pallas_call(
        localize_kernel,
        out_shape=jax.ShapeDtypeStruct((kinds, levels, rows, width), jnp.float32),
        in_specs=[pl.BlockSpec(memory_space=pltpu.VMEM)] * 4,
        out_specs=pl.BlockSpec(memory_space=pltpu.VMEM),
        scratch_shapes=[
            pltpu.VMEM((count, fields, rows, depth), low),
            pltpu.VMEM((count, rows, count * rows), low),
            pltpu.VMEM((count, fields, rows, depth), low),
            pltpu.VMEM((mems, count, fields, rows, depth), low),
            pltpu.VMEM((count, depth, width), low),
            pltpu.VMEM((mems, kinds, members, levels, rows, width), low),
            pltpu.VMEM((mems * fields * rows, width), jnp.float32),
            dma((count,)), dma((count,)), dma((count,)), dma((count,)), dma((count,)), dma((count,)),
            dma((mems, count)), dma((mems, count)), dma((mems,)), dma((mems,)),
            dma((chains, count)), dma((chains, count)),
            dma((chains, count, levs)), dma((chains, count, levs)), dma((2,)),
        ],
        compiler_params=pltpu.CompilerParams(
            collective_id=0, has_side_effects=True, vmem_limit_bytes=56 << 20
        ),
        name="localize",
    )(split, perturbations, column_taper, row_taper)


def on_device(
    control_fields, perturbations, column_taper, row_taper, courant_numbers, tracer_slope
):
    weighted = localized(control_fields, perturbations, column_taper, row_taper)
    return advected(weighted, courant_numbers, tracer_slope)


def solution(mesh):
    placed = (
        P("mem", "lev", "row", None),
        P(None, "mem", "lev", "row", None),
        P("row", None),
        P("row", None),
        P(None, "lev", "row", "mem"),
        P(None, "lev", "row", "mem"),
    )
    return jax.shard_map(
        on_device,
        mesh=mesh,
        in_specs=placed,
        out_specs=P(None, "lev", "row", "mem"),
        check_vma=False,
    )
```
